32 devices in a mesh: grp: 2 (over y), brick: 4 (over z), vec: 2 (over x), sub: 2 (over core).
Axes of the slice: x: 2, y: 2, z: 4, core: 2. Of those that a mesh axis runs over, the one named last changes fastest.
Arguments:
- vectors: float32 [128, 3, 2, 16384], P(('vec', 'sub'), None, None, ('grp', 'brick')), parts along dimension 3, may hold values from -6 to 6
- gauge_links: float32 [3, 3, 3, 2, 16384], P(None, None, None, None, ('grp', 'brick')), parts along dimension 4, may hold values from -1 to 1, as said below
- momenta: int32 [27, 3], replicated, may hold values from -3 to 3
Outputs:
- elementals: float32 [128, 54, 2, 128], P(('vec', 'sub'), 'grp', None, 'brick'), parts along dimension 1
The draws below stay inside these ranges and needn't reach their ends.
There are 2 independent parts, one for each index of `grp`. The reference program is written for one: setup_inputs(seed, part) draws one part's arguments, and reference() takes and returns one part's arrays. A program takes and returns all parts, laid end to end along the dimension named above; an argument that names none is the same for every part. Nothing has to cross between parts.
Inputs may be any that keep to these rules, and one draw needn't show every extreme that they name: Each gauge_links[mu, :, :, :, s] is a unitary 3x3 complex matrix.
All inputs are finite; a program needn't handle non-finite values.
Results may differ from the reference program's by a relative error of at most 0.0049.
Values may be sent and summed in bfloat16 or wider, within the bound.
A program may use at most 128 MiB of HBM per device.

```python
import math
import jax
import jax.numpy as jnp
from jax import lax

NV = 128
P_SIZE = 27
LY = 64
LZ = 8
ITERS = 2
NX = 16
SITES = 8192


def inner_product(first, second):
    real_part = jnp.sum(first[:, :, 0] * second[:, :, 0] + first[:, :, 1] * second[:, :, 1], axis=1)
    imag_part = jnp.sum(first[:, :, 0] * second[:, :, 1] - first[:, :, 1] * second[:, :, 0], axis=1)
    return (real_part[:, None], imag_part[:, None])


def remove_along(first, second):
    real_part, imag_part = inner_product(first, second)
    new_real = second[:, :, 0] - (real_part * first[:, :, 0] - imag_part * first[:, :, 1])
    new_imag = second[:, :, 1] - (real_part * first[:, :, 1] + imag_part * first[:, :, 0])
    return jnp.stack([new_real, new_imag], axis=2)


def normalize(matrix_row):
    length = jnp.sum(matrix_row * matrix_row, axis=(1, 2))
    return matrix_row * jax.lax.rsqrt(length + 1e-06)[:, None, None, :]


def draw_gauge_links(key, part):
    noise = jax.random.normal(jax.random.fold_in(key, 7), (3, 3, 3, 2, SITES), jnp.float32)
    first = normalize(noise[:, 0])
    second = normalize(remove_along(first, noise[:, 1]))
    third = remove_along(second, remove_along(first, noise[:, 2]))
    third = normalize(third)
    return jnp.stack([first, second, third], axis=1)


def place_ends(values, own_key, least, largest):
    place = [jax.random.randint(jax.random.fold_in(own_key, axis), (), 0, length) for axis, length in enumerate(values.shape)]
    widest = values.shape.index(max(values.shape))
    next_to = place[:widest] + [(place[widest] + 1) % values.shape[widest]] + place[widest + 1:]
    return values.at[tuple(place)].set(least).at[tuple(next_to)].set(largest)


def steps_of(rng, shape, cuts, smallest, top_value):
    loudness, own = 1.0, jax.random.fold_in(rng, 6)
    for position, parts in cuts:
        heights = jnp.exp(jax.random.uniform(jax.random.fold_in(own, position), (parts,), jnp.float32, smallest / len(cuts), top_value / len(cuts)))
        loudness = loudness * jnp.repeat(heights, shape[position] // parts).reshape([-1 if axis == position else 1 for axis in range(len(shape))])
    return loudness


def scatter_about(key, shape, width, reach, cuts=(), held_as=jnp.bfloat16):
    result = width * jax.random.normal(key, shape, jnp.float32)
    if cuts:
        result = result * steps_of(key, shape, cuts, -0.22, 0.18)
    return jnp.clip(result, -reach, reach).astype(held_as)


def setup_inputs(seed: int = 0, part: int = 0) -> dict:
    keys = jax.random.split(jax.random.key(seed), 4)
    part_keys = jax.random.split(jax.random.fold_in(keys[3], part), 4)
    vectors = scatter_about(part_keys[0], (NV, 3, 2, SITES), 1.0, 6.0, ((0, 4), (3, 4)), jnp.float32)
    gauge_links = draw_gauge_links(jax.random.fold_in(jax.random.fold_in(keys[3], part), 71), part)
    momenta = place_ends(jax.random.randint(keys[2], (P_SIZE, 3), -3, 4), jax.random.fold_in(keys[2], 1), -3, 3).astype(jnp.int32)
    return {"vectors": vectors, "gauge_links": gauge_links, "momenta": momenta}


KAPPA = 0.125


def matrix_apply(matrix, source):
    matrix_real = matrix[:, :, 0][None]
    matrix_imag = matrix[:, :, 1][None]
    source_real = source[:, None, :, 0]
    source_imag = source[:, None, :, 1]
    real_part = jnp.sum(matrix_real * source_real - matrix_imag * source_imag, axis=2)
    imag_part = jnp.sum(matrix_real * source_imag + matrix_imag * source_real, axis=2)
    return jnp.stack([real_part, imag_part], axis=2)


def adjoint(matrix):
    return jnp.stack([jnp.swapaxes(matrix[:, :, 0], 0, 1), -jnp.swapaxes(matrix[:, :, 1], 0, 1)], axis=2)


def smear_step(field, gauge):
    total = None
    for direction in range(3):
        axis = 3 + direction
        forward = matrix_apply(gauge[direction], jnp.roll(field, -1, axis=axis))
        behind = adjoint(jnp.roll(gauge[direction], 1, axis=axis))
        backward = matrix_apply(behind, jnp.roll(field, 1, axis=axis))
        term = forward + backward
        total = term if total is None else total + term
    return field + KAPPA * (total - 6.0 * field)


def reference(vectors, gauge_links, momenta):
    field = vectors.reshape((NV, 3, 2, NX, LY, LZ))
    gauge = gauge_links.reshape((3, 3, 3, 2, NX, LY, LZ))
    for step in range(ITERS):
        field = smear_step(field, gauge)
    smeared_low = field.reshape((NV, 3, 2, SITES)).astype(jnp.bfloat16)
    smeared_wide = lax.optimization_barrier(smeared_low).astype(jnp.float32)
    raw_wide = lax.optimization_barrier(vectors.astype(jnp.bfloat16)).astype(jnp.float32)
    right = smeared_wide.reshape((NV, 6 * SITES))
    site = jnp.arange(SITES, dtype=jnp.int32)
    layer_index = site // (LY * LZ)
    column_index = (site // LZ) % LY
    depth_index = site % LZ

    def one_momentum(triple):
        fraction = (jnp.mod(triple[0] * layer_index, NX).astype(jnp.float32) / NX
                    + jnp.mod(triple[1] * column_index, LY).astype(jnp.float32) / LY
                    + jnp.mod(triple[2] * depth_index, LZ).astype(jnp.float32) / LZ)
        angle = (2.0 * math.pi) * fraction
        cosine = jnp.cos(angle)
        sine = jnp.sin(angle)
        real_part = raw_wide[:, :, 0] * cosine - raw_wide[:, :, 1] * sine
        imag_part = raw_wide[:, :, 0] * sine + raw_wide[:, :, 1] * cosine
        phased = jnp.stack([real_part, imag_part], axis=2).astype(jnp.bfloat16)
        phased = lax.optimization_barrier(phased).astype(jnp.float32)
        turned = jnp.stack([-phased[:, :, 1], phased[:, :, 0]], axis=2)
        left = jnp.concatenate([phased.reshape((NV, 6 * SITES)), turned.reshape((NV, 6 * SITES))], axis=0)
        product = lax.dot_general(left, right, (((1,), (1,)), ((), ())),
                                  precision=lax.Precision.HIGHEST, preferred_element_type=jnp.float32)
        return product.reshape((2, NV, NV))

    blocks = lax.map(one_momentum, momenta)
    scale = (3.0 * SITES) ** -0.5
    return jnp.transpose(blocks, (2, 0, 1, 3)) * scale
```

```python
import functools
import math

import jax
import jax.numpy as jnp
from jax import lax
from jax.experimental import pallas as pl
from jax.experimental.pallas import tpu as pltpu
from jax.sharding import PartitionSpec as P

LY = 64
LZ = 8
ITERS = 2


KAPPA = 0.125


def from_behind(array, axis, by):
    peers = lax.axis_size(axis)
    return lax.ppermute(array, axis, [(i, (i + by) % peers) for i in range(peers)])


def padded_2(array, sides, width):
    for axis, dim in sides:
        peers, length = (lax.axis_size(axis), array.shape[dim])
        up = [(i, (i + 1) % peers) for i in range(peers)]
        down = [(j, i) for i, j in up]
        last = lax.slice_in_dim(array, length - width, length, axis=dim)
        initial = lax.slice_in_dim(array, 0, width, axis=dim)
        before = lax.ppermute(last, axis, up)
        after = lax.ppermute(initial, axis, down)
        array = jnp.concatenate([before, array, after], axis=dim)
    return array


def matrix_apply(matrix, source):
    matrix_real = matrix[:, :, 0][None]
    matrix_imag = matrix[:, :, 1][None]
    source_real = source[:, None, :, 0]
    source_imag = source[:, None, :, 1]
    real_part = jnp.sum(matrix_real * source_real - matrix_imag * source_imag, axis=2)
    imag_part = jnp.sum(matrix_real * source_imag + matrix_imag * source_real, axis=2)
    return jnp.stack([real_part, imag_part], axis=2)


def adjoint(matrix):
    return jnp.stack(
        [jnp.swapaxes(matrix[:, :, 0], 0, 1), -jnp.swapaxes(matrix[:, :, 1], 0, 1)], axis=2
    )


def step_depth(values, offset):
    depth_index = lax.iota(jnp.int32, values.shape[-1]) % LZ
    if offset > 0:
        return jnp.where(
            depth_index == LZ - 1, jnp.roll(values, LZ - 1, -1), jnp.roll(values, -1, -1)
        )
    return jnp.where(depth_index == 0, jnp.roll(values, 1 - LZ, -1), jnp.roll(values, 1, -1))


def step_column(values, offset):
    plane = LY * LZ
    column_index = lax.iota(jnp.int32, values.shape[-1]) // LZ % LY
    if offset > 0:
        return jnp.where(
            column_index == LY - 1, jnp.roll(values, plane - LZ, -1), jnp.roll(values, -LZ, -1)
        )
    return jnp.where(column_index == 0, jnp.roll(values, LZ - plane, -1), jnp.roll(values, LZ, -1))


def laplace_step(center, ahead, behind, here_links, back_links):
    forward = matrix_apply(here_links[0], ahead)
    backward = matrix_apply(adjoint(back_links), behind)
    total = forward + backward
    for direction, stepper in ((1, step_column), (2, step_depth)):
        forward = matrix_apply(here_links[direction], stepper(center, 1))
        backward = matrix_apply(adjoint(stepper(here_links[direction], -1)), stepper(center, -1))
        total = total + (forward + backward)
    return center + KAPPA * (total - 6.0 * center)


def shards(vectors, gauge_links, momenta):
    plane = LY * LZ
    local_sites = vectors.shape[3]
    raw_low = vectors.astype(jnp.bfloat16)
    field = vectors
    x_links = gauge_links[0]
    rim = from_behind(x_links[..., local_sites - plane :], "brick", 1)
    back_links = jnp.concatenate([rim, x_links[..., : local_sites - plane]], axis=3)
    for step in range(ITERS):
        padded = padded_2(field, (("brick", 3),), plane)
        field = laplace_step(
            padded[..., plane : plane + local_sites],
            padded[..., 2 * plane :],
            padded[..., :local_sites],
            gauge_links,
            back_links,
        )
    smeared_low = field.astype(jnp.bfloat16)
    raw_sites, smeared_sites = (
        lax.all_to_all(raw_low, ("vec", "sub"), split_axis=3, concat_axis=0, tiled=True),
        lax.all_to_all(smeared_low, ("vec", "sub"), split_axis=3, concat_axis=0, tiled=True),
    )
    groups = lax.axis_size(("vec", "sub"))
    total_vec = raw_sites.shape[0]
    width = raw_sites.shape[3]
    total_x = lax.axis_size("brick") * (local_sites // plane)
    first_site = lax.axis_index("brick") * local_sites + lax.axis_index(("vec", "sub")) * width
    site = first_site + lax.iota(jnp.int32, width)
    layer_index = (site // plane)[None]
    column_index = (site // LZ % LY)[None]
    depth_index = (site % LZ)[None]
    fraction = (
        jnp.mod(momenta[:, 0:1] * layer_index, total_x).astype(jnp.float32) / total_x
        + jnp.mod(momenta[:, 1:2] * column_index, LY).astype(jnp.float32) / LY
        + jnp.mod(momenta[:, 2:3] * depth_index, LZ).astype(jnp.float32) / LZ
    )
    angle = 2.0 * math.pi * fraction
    cosines = jnp.cos(angle)
    sines = jnp.sin(angle)
    right = smeared_sites.reshape((total_vec, 6 * width))
    scale = (3.0 * total_x * plane) ** (-0.5)

    def one_momentum(angles):
        cosine, sine = angles
        real_part = raw_sites[:, :, 0] * cosine - raw_sites[:, :, 1] * sine
        imag_part = raw_sites[:, :, 0] * sine + raw_sites[:, :, 1] * cosine
        phased = jnp.stack([real_part, imag_part], axis=2).astype(jnp.bfloat16)
        turned = jnp.stack([-phased[:, :, 1], phased[:, :, 0]], axis=2)
        left = jnp.concatenate(
            [
                phased.reshape((lax.axis_size(("vec", "sub")) * (total_vec // groups), 6 * width)),
                turned.reshape((lax.axis_size(("vec", "sub")) * (total_vec // groups), 6 * width)),
            ],
            axis=0,
        )
        product = lax.dot_general(
            left, right, (((1,), (1,)), ((), ())), preferred_element_type=jnp.float32
        )
        return product.reshape(
            (2, lax.axis_size(("vec", "sub")) * (total_vec // groups), total_vec)
        )

    blocks = lax.map(one_momentum, (cosines, sines))
    shares = lax.psum_scatter(
        jnp.transpose(blocks, (2, 0, 1, 3)) * scale, ("vec", "sub"), scatter_dimension=0, tiled=True
    )
    return lax.psum_scatter(shares, "brick", scatter_dimension=3, tiled=True)


def smear_kernel(planes, rows, x_ref, lo_ref, hi_ref, lk_ref, lb_ref, la_ref, out_ref, stage, table, f0, f1, moved):
    plane = LY * LZ
    f32 = jnp.float32
    blocks = rows // 8
    depth = lax.broadcasted_iota(jnp.int32, (8, plane), 1) % LZ
    link_depth = lax.broadcasted_iota(jnp.int32, (56, plane), 1) % LZ

    for k in range(6):
        f0[k] = lo_ref[k].astype(f32)
        f0[6 + 3 * planes + k] = hi_ref[k].astype(f32)

    def take(k, carry):
        f0[6 + k] = x_ref[k]
        return carry

    lax.fori_loop(0, 3 * planes, take, 0)
    for k in range(2):
        stage[k, 0:54] = lb_ref[k].astype(f32)
    for k in range(planes):
        stage[2 + k, 0:54] = lk_ref[k]
    stage[2 + planes, 0:54] = la_ref[0].astype(f32)

    def spread(t, carry):
        here = stage[t + 1]
        behind_x = stage[t]
        behind_y = pltpu.roll(here, LZ, 1)
        behind_z = jnp.where(
            link_depth == 0, pltpu.roll(here, plane - (LZ - 1), 1), pltpu.roll(here, 1, 1)
        )
        for r in range(54):
            table[t, r] = jnp.broadcast_to(here[r : r + 1], (8, plane))
            back = (behind_x, behind_y, behind_z)[r // 18]
            table[t, 54 + r] = jnp.broadcast_to(back[r : r + 1], (8, plane))
        return carry

    lax.fori_loop(0, planes + 2, spread, 0)

    def one_plane(source, at, links, target, to):
        def shift(k, carry):
            c, b = k // blocks, k % blocks
            rows_at = pl.ds(pl.multiple_of(b * 8, 8), 8)
            for half in range(2):
                lanes = slice(half * plane, (half + 1) * plane)
                v = source[at * 3 + c, rows_at, lanes]
                moved[0, c, rows_at, lanes] = pltpu.roll(v, plane - LZ, 1)
                moved[1, c, rows_at, lanes] = pltpu.roll(v, LZ, 1)
                moved[2, c, rows_at, lanes] = jnp.where(
                    depth == LZ - 1, pltpu.roll(v, LZ - 1, 1), pltpu.roll(v, plane - 1, 1)
                )
                moved[3, c, rows_at, lanes] = jnp.where(
                    depth == 0, pltpu.roll(v, plane - (LZ - 1), 1), pltpu.roll(v, 1, 1)
                )
            return carry

        lax.fori_loop(0, 3 * blocks, shift, 0)

        def block(k, carry):
            b, lane = k % blocks, k // blocks
            rows_at = pl.ds(pl.multiple_of(b * 8, 8), 8)
            real_at = pl.ds(pl.multiple_of(lane * 128, 128), 128)
            imag_at = pl.ds(pl.multiple_of(plane + lane * 128, 128), 128)
            acc = [[None, None] for _ in range(3)]

            def add(r, part, value):
                acc[r][part] = value if acc[r][part] is None else acc[r][part] + value

            for way in range(6):
                direction, back = way // 2, way % 2
                for c in range(3):
                    if direction == 0:
                        index = (at + 1 - 2 * back) * 3 + c
                        sr = source[index, rows_at, real_at]
                        si = source[index, rows_at, imag_at]
                    else:
                        sr = moved[way - 2, c, rows_at, real_at]
                        si = moved[way - 2, c, rows_at, imag_at]
                    for r in range(3):
                        row = direction * 18 + (54 + c * 6 + r * 2 if back else r * 6 + c * 2)
                        ur = table[links, row, :, real_at]
                        ui = table[links, row + 1, :, real_at]
                        if back:
                            add(r, 0, ur * sr + ui * si)
                            add(r, 1, ur * si - ui * sr)
                        else:
                            add(r, 0, ur * sr - ui * si)
                            add(r, 1, ur * si + ui * sr)
            for r in range(3):
                for part, lanes in ((0, real_at), (1, imag_at)):
                    mid = source[at * 3 + r, rows_at, lanes]
                    target[to * 3 + r, rows_at, lanes] = mid + KAPPA * (acc[r][part] - 6.0 * mid)
            return carry

        lax.fori_loop(0, blocks * (plane // 128), block, 0)

    def first(t, carry):
        one_plane(f0, t + 1, t, f1, t)
        return carry

    lax.fori_loop(0, planes + 2, first, 0)

    def second(t, carry):
        one_plane(f1, t + 1, t + 1, f0, t)
        return carry

    lax.fori_loop(0, planes, second, 0)

    def put(k, carry):
        out_ref[k] = f0[k].astype(out_ref.dtype)
        return carry

    lax.fori_loop(0, 3 * planes, put, 0)


def product_kernel(groups, rows, count, scale, order_ref, cos_ref, sin_ref, smeared_ref, *rest):
    plane = LY * LZ
    raw_refs = rest[:groups]
    out_refs = rest[groups : 2 * groups]
    right, left, wide, total = rest[2 * groups :]
    total[...] = jnp.zeros_like(total)

    def chunk(k, carry):
        for u in range(groups):
            raw = raw_refs[u][k]
            first = 2 * rows * u
            right[first : first + rows, :] = raw
            right[first + rows : first + 2 * rows, 0:plane] = -raw[:, plane:]
            right[first + rows : first + 2 * rows, plane:] = raw[:, :plane]
        wide[...] = smeared_ref[k].astype(jnp.float32)

        def turn(q, carry):
            cosine = cos_ref[k // 3, pl.ds(q, 1), :]
            sine = sin_ref[k // 3, pl.ds(q, 1), :]
            sr = wide[:, 0:plane]
            si = wide[:, plane:]
            at = pl.ds(pl.multiple_of(q * rows, rows), rows)
            left[at, 0:plane] = (cosine * sr + sine * si).astype(left.dtype)
            left[at, plane:] = (cosine * si - sine * sr).astype(left.dtype)
            return carry

        lax.fori_loop(0, count, turn, 0)
        total[...] += lax.dot_general(
            right[...], left[...], (((1,), (1,)), ((), ())), preferred_element_type=jnp.float32
        )
        return carry

    lax.fori_loop(0, smeared_ref.shape[0], chunk, 0)
    for k in range(groups):
        first = pl.multiple_of(order_ref[k] * (2 * rows), 2 * rows)
        out_refs[k][...] = (total[pl.ds(first, 2 * rows), :] * scale).astype(out_refs[k].dtype)


def phase_tables(momenta, local_sites, total_x):
    plane = LY * LZ
    site = lax.axis_index("brick") * local_sites + lax.iota(jnp.int32, local_sites)
    site = site.reshape((local_sites // plane, 1, plane))
    fraction = (
        jnp.mod(momenta[None, :, 0:1] * (site // plane), total_x).astype(jnp.float32) / total_x
        + jnp.mod(momenta[None, :, 1:2] * (site // LZ % LY), LY).astype(jnp.float32) / LY
        + jnp.mod(momenta[None, :, 2:3] * (site % LZ), LZ).astype(jnp.float32) / LZ
    )
    angle = 2.0 * math.pi * fraction
    return jnp.cos(angle), jnp.sin(angle)


def shards_kernels(vectors, gauge_links, momenta):
    plane = LY * LZ
    rows, local_sites = vectors.shape[0], vectors.shape[3]
    planes = local_sites // plane
    bricks, vecs, subs = (lax.axis_size(a) for a in ("brick", "vec", "sub"))
    groups = vecs * subs
    count = momenta.shape[0]
    low = jnp.bfloat16
    wide = jnp.transpose(vectors.reshape((rows, 3, 2, planes, plane)), (3, 1, 0, 2, 4))
    wide = wide.reshape((planes * 3, rows, 2 * plane))
    raw = wide.astype(low)
    below = from_behind(raw[-6:], "brick", 1)
    above = from_behind(raw[:6], "brick", -1)
    links = jnp.transpose(gauge_links.reshape((54, planes, plane)), (1, 0, 2))
    links_low = links.astype(low)
    links_below = from_behind(links_low[-2:], "brick", 1)
    links_above = from_behind(links_low[:1], "brick", -1)
    gathered = []
    for kv in range(vecs):
        one = raw if kv == 0 else from_behind(raw, "vec", -kv)
        for ks in range(subs):
            gathered.append(one if ks == 0 else from_behind(one, "sub", -ks))
    cosines, sines = phase_tables(momenta, local_sites, bricks * planes)

    vmem = pl.BlockSpec(memory_space=pltpu.VMEM)
    smeared = pl.pallas_call(
        functools.partial(smear_kernel, planes, rows),
        out_shape=jax.ShapeDtypeStruct((planes * 3, rows, 2 * plane), low),
        in_specs=[vmem] * 6,
        out_specs=vmem,
        scratch_shapes=[
            pltpu.VMEM((planes + 3, 56, plane), jnp.float32),
            pltpu.VMEM((planes + 2, 108, 8, plane), jnp.float32),
            pltpu.VMEM(((planes + 4) * 3, rows, 2 * plane), jnp.float32),
            pltpu.VMEM(((planes + 2) * 3, rows, 2 * plane), jnp.float32),
            pltpu.VMEM((4, 3, rows, 2 * plane), jnp.float32),
        ],
        compiler_params=pltpu.CompilerParams(vmem_limit_bytes=48 * 2**20),
        cost_estimate=pl.CostEstimate(
            flops=432 * 2 * (planes + 1) * plane * rows * 4, bytes_accessed=4 * 2**20, transcendentals=0
        ),
        name="smear",
    )(wide, below, above, links, links_below, links_above)

    me_vec, me_sub, me_brick = (lax.axis_index(a) for a in ("vec", "sub", "brick"))
    owner = (me_brick + lax.iota(jnp.int32, groups)) % groups
    order = (owner // subs - me_vec) % vecs * subs + (owner % subs - me_sub) % subs
    scale = (3.0 * bricks * local_sites) ** (-0.5)
    blocks = pl.pallas_call(
        functools.partial(product_kernel, groups, rows, count, scale),
        out_shape=[jax.ShapeDtypeStruct((2 * rows, count * rows), low)] * groups,
        in_specs=[pl.BlockSpec(memory_space=pltpu.SMEM)] + [vmem] * (3 + groups),
        out_specs=[vmem] * groups,
        scratch_shapes=[
            pltpu.VMEM((2 * rows * groups, 2 * plane), low),
            pltpu.VMEM((count * rows, 2 * plane), low),
            pltpu.VMEM((rows, 2 * plane), jnp.float32),
            pltpu.VMEM((2 * rows * groups, count * rows), jnp.float32),
        ],
        compiler_params=pltpu.CompilerParams(vmem_limit_bytes=40 * 2**20),
        cost_estimate=pl.CostEstimate(
            flops=2 * 2 * rows * groups * count * rows * 6 * local_sites,
            bytes_accessed=8 * 2**20,
            transcendentals=0,
        ),
        name="product",
    )(order, cosines, sines, smeared, *gathered)

    total = None
    for k in range(groups):
        pairs = [
            (b * groups + u, u * groups + (b + k) % groups)
            for b in range(bricks)
            for u in range(groups)
        ]
        got = lax.ppermute(blocks[k], ("brick", "vec", "sub"), pairs).astype(jnp.float32)
        total = got if total is None else total + got
    return jnp.transpose(total.reshape((2, rows, count, rows)), (1, 2, 0, 3))


def choose(vectors, gauge_links, momenta):
    groups = lax.axis_size(("vec", "sub"))
    planes = vectors.shape[3] // (LY * LZ)
    if groups == lax.axis_size("brick") and planes >= 2 and vectors.shape[0] % 16 == 0:
        return shards_kernels(vectors, gauge_links, momenta)
    return shards(vectors, gauge_links, momenta)


def solution(mesh):
    in_specs = (
        P(("vec", "sub"), None, None, ("grp", "brick")),
        P(None, None, None, None, ("grp", "brick")),
        P(),
    )
    out_specs = P(("vec", "sub"), "grp", None, "brick")
    return jax.shard_map(choose, mesh=mesh, in_specs=in_specs, out_specs=out_specs, check_vma=False)
```

```python
import functools
import math

import jax
import jax.numpy as jnp
from jax import lax
from jax.experimental import pallas as pl
from jax.experimental.pallas import tpu as pltpu
from jax.sharding import PartitionSpec as P

LY = 64
LZ = 8
ITERS = 2


KAPPA = 0.125


def from_behind(array, axis, by):
    peers = lax.axis_size(axis)
    return lax.ppermute(array, axis, [(i, (i + by) % peers) for i in range(peers)])


def padded_2(array, sides, width):
    for axis, dim in sides:
        peers, length = (lax.axis_size(axis), array.shape[dim])
        up = [(i, (i + 1) % peers) for i in range(peers)]
        down = [(j, i) for i, j in up]
        last = lax.slice_in_dim(array, length - width, length, axis=dim)
        initial = lax.slice_in_dim(array, 0, width, axis=dim)
        before = lax.ppermute(last, axis, up)
        after = lax.ppermute(initial, axis, down)
        array = jnp.concatenate([before, array, after], axis=dim)
    return array


def matrix_apply(matrix, source):
    matrix_real = matrix[:, :, 0][None]
    matrix_imag = matrix[:, :, 1][None]
    source_real = source[:, None, :, 0]
    source_imag = source[:, None, :, 1]
    real_part = jnp.sum(matrix_real * source_real - matrix_imag * source_imag, axis=2)
    imag_part = jnp.sum(matrix_real * source_imag + matrix_imag * source_real, axis=2)
    return jnp.stack([real_part, imag_part], axis=2)


def adjoint(matrix):
    return jnp.stack(
        [jnp.swapaxes(matrix[:, :, 0], 0, 1), -jnp.swapaxes(matrix[:, :, 1], 0, 1)], axis=2
    )


def step_depth(values, offset):
    depth_index = lax.iota(jnp.int32, values.shape[-1]) % LZ
    if offset > 0:
        return jnp.where(
            depth_index == LZ - 1, jnp.roll(values, LZ - 1, -1), jnp.roll(values, -1, -1)
        )
    return jnp.where(depth_index == 0, jnp.roll(values, 1 - LZ, -1), jnp.roll(values, 1, -1))


def step_column(values, offset):
    plane = LY * LZ
    column_index = lax.iota(jnp.int32, values.shape[-1]) // LZ % LY
    if offset > 0:
        return jnp.where(
            column_index == LY - 1, jnp.roll(values, plane - LZ, -1), jnp.roll(values, -LZ, -1)
        )
    return jnp.where(column_index == 0, jnp.roll(values, LZ - plane, -1), jnp.roll(values, LZ, -1))


def laplace_step(center, ahead, behind, here_links, back_links):
    forward = matrix_apply(here_links[0], ahead)
    backward = matrix_apply(adjoint(back_links), behind)
    total = forward + backward
    for direction, stepper in ((1, step_column), (2, step_depth)):
        forward = matrix_apply(here_links[direction], stepper(center, 1))
        backward = matrix_apply(adjoint(stepper(here_links[direction], -1)), stepper(center, -1))
        total = total + (forward + backward)
    return center + KAPPA * (total - 6.0 * center)


def shards(vectors, gauge_links, momenta):
    plane = LY * LZ
    local_sites = vectors.shape[3]
    raw_low = vectors.astype(jnp.bfloat16)
    field = vectors
    x_links = gauge_links[0]
    rim = from_behind(x_links[..., local_sites - plane :], "brick", 1)
    back_links = jnp.concatenate([rim, x_links[..., : local_sites - plane]], axis=3)
    for step in range(ITERS):
        padded = padded_2(field, (("brick", 3),), plane)
        field = laplace_step(
            padded[..., plane : plane + local_sites],
            padded[..., 2 * plane :],
            padded[..., :local_sites],
            gauge_links,
            back_links,
        )
    smeared_low = field.astype(jnp.bfloat16)
    raw_sites, smeared_sites = (
        lax.all_to_all(raw_low, ("vec", "sub"), split_axis=3, concat_axis=0, tiled=True),
        lax.all_to_all(smeared_low, ("vec", "sub"), split_axis=3, concat_axis=0, tiled=True),
    )
    groups = lax.axis_size(("vec", "sub"))
    total_vec = raw_sites.shape[0]
    width = raw_sites.shape[3]
    total_x = lax.axis_size("brick") * (local_sites // plane)
    first_site = lax.axis_index("brick") * local_sites + lax.axis_index(("vec", "sub")) * width
    site = first_site + lax.iota(jnp.int32, width)
    layer_index = (site // plane)[None]
    column_index = (site // LZ % LY)[None]
    depth_index = (site % LZ)[None]
    fraction = (
        jnp.mod(momenta[:, 0:1] * layer_index, total_x).astype(jnp.float32) / total_x
        + jnp.mod(momenta[:, 1:2] * column_index, LY).astype(jnp.float32) / LY
        + jnp.mod(momenta[:, 2:3] * depth_index, LZ).astype(jnp.float32) / LZ
    )
    angle = 2.0 * math.pi * fraction
    cosines = jnp.cos(angle)
    sines = jnp.sin(angle)
    right = smeared_sites.reshape((total_vec, 6 * width))
    scale = (3.0 * total_x * plane) ** (-0.5)

    def one_momentum(angles):
        cosine, sine = angles
        real_part = raw_sites[:, :, 0] * cosine - raw_sites[:, :, 1] * sine
        imag_part = raw_sites[:, :, 0] * sine + raw_sites[:, :, 1] * cosine
        phased = jnp.stack([real_part, imag_part], axis=2).astype(jnp.bfloat16)
        turned = jnp.stack([-phased[:, :, 1], phased[:, :, 0]], axis=2)
        left = jnp.concatenate(
            [
                phased.reshape((lax.axis_size(("vec", "sub")) * (total_vec // groups), 6 * width)),
                turned.reshape((lax.axis_size(("vec", "sub")) * (total_vec // groups), 6 * width)),
            ],
            axis=0,
        )
        product = lax.dot_general(
            left, right, (((1,), (1,)), ((), ())), preferred_element_type=jnp.float32
        )
        return product.reshape(
            (2, lax.axis_size(("vec", "sub")) * (total_vec // groups), total_vec)
        )

    blocks = lax.map(one_momentum, (cosines, sines))
    shares = lax.psum_scatter(
        jnp.transpose(blocks, (2, 0, 1, 3)) * scale, ("vec", "sub"), scatter_dimension=0, tiled=True
    )
    return lax.psum_scatter(shares, "brick", scatter_dimension=3, tiled=True)


def smear_kernel(planes, rows, x_ref, lo_ref, hi_ref, lk_ref, out_ref, stage, table, f0, f1, moved):
    plane = LY * LZ
    f32 = jnp.float32
    blocks = rows // 8
    depth = lax.broadcasted_iota(jnp.int32, (8, 128), 1) % LZ
    link_depth = lax.broadcasted_iota(jnp.int32, (stage.shape[1], plane), 1) % LZ

    for k in range(6):
        f0[k] = lo_ref[k].astype(f32)
        f0[6 + 3 * planes + k] = hi_ref[k].astype(f32)

    def take(k, carry):
        f0[6 + k] = x_ref[k]
        return carry

    lax.fori_loop(0, 3 * planes, take, 0)
    for j in range(stage.shape[1] // rows):
        at = slice(j * rows, (j + 1) * rows)
        stage[0, at] = lo_ref[6 + j, :, 0:plane].astype(f32)
        stage[1, at] = lo_ref[6 + j, :, plane:].astype(f32)
        stage[2 + planes, at] = hi_ref[6 + j, :, 0:plane].astype(f32)
    for k in range(planes):
        stage[2 + k, 0:54] = lk_ref[:, k * plane : (k + 1) * plane]

    def spread(t, carry):
        here = stage[t + 1]
        behind_x = stage[t]
        behind_y = pltpu.roll(here, LZ, 1)
        behind_z = jnp.where(
            link_depth == 0, pltpu.roll(here, plane - (LZ - 1), 1), pltpu.roll(here, 1, 1)
        )
        for r in range(54):
            table[t, r] = jnp.broadcast_to(here[r : r + 1], (8, plane))
            back = (behind_x, behind_y, behind_z)[r // 18]
            table[t, 54 + r] = jnp.broadcast_to(back[r : r + 1], (8, plane))
        return carry

    lax.fori_loop(0, planes + 2, spread, 0)

    def one_plane(source, at, links, target, to):
        def shift(k, carry):
            c, half = k // 2, k % 2
            for b in range(blocks):
                rows_at = slice(b * 8, b * 8 + 8)
                lanes = pl.ds(pl.multiple_of(half * plane, plane), plane)
                v = source[at * 3 + c, rows_at, lanes]
                moved[0, c, rows_at, lanes] = pltpu.roll(v, plane - LZ, 1)
                moved[1, c, rows_at, lanes] = pltpu.roll(v, LZ, 1)
                for part in range(plane // 128):
                    w = v[:, part * 128 : part * 128 + 128]
                    here = pl.ds(pl.multiple_of(half * plane + part * 128, 128), 128)
                    moved[2, c, rows_at, here] = jnp.where(
                        depth == LZ - 1, pltpu.roll(w, LZ - 1, 1), pltpu.roll(w, 127, 1)
                    )
                    moved[3, c, rows_at, here] = jnp.where(
                        depth == 0, pltpu.roll(w, 128 - (LZ - 1), 1), pltpu.roll(w, 1, 1)
                    )
            return carry

        lax.fori_loop(0, 6, shift, 0)

        def block(lane, carry):
            lanes = (
                pl.ds(pl.multiple_of(lane * 128, 128), 128),
                pl.ds(pl.multiple_of(plane + lane * 128, 128), 128),
            )
            acc = {}

            def add(b, r, part, value):
                acc[b, r, part] = value + acc[b, r, part] if (b, r, part) in acc else value

            for way in range(6):
                direction, back = way // 2, way % 2
                for c in range(3):
                    pair = []
                    for r in range(3):
                        row = direction * 18 + (54 + c * 6 + r * 2 if back else r * 6 + c * 2)
                        pair.append((table[links, row, :, lanes[0]], table[links, row + 1, :, lanes[0]]))
                    for b in range(blocks):
                        at_rows = slice(b * 8, b * 8 + 8)
                        if direction == 0:
                            index = (at + 1 - 2 * back) * 3 + c
                            sr = source[index, at_rows, lanes[0]]
                            si = source[index, at_rows, lanes[1]]
                        else:
                            sr = moved[way - 2, c, at_rows, lanes[0]]
                            si = moved[way - 2, c, at_rows, lanes[1]]
                        for r, (ur, ui) in enumerate(pair):
                            if back:
                                add(b, r, 0, ur * sr + ui * si)
                                add(b, r, 1, ur * si - ui * sr)
                            else:
                                add(b, r, 0, ur * sr - ui * si)
                                add(b, r, 1, ur * si + ui * sr)
            for (b, r, part), value in acc.items():
                at_rows = slice(b * 8, b * 8 + 8)
                mid = source[at * 3 + r, at_rows, lanes[part]]
                target[to * 3 + r, at_rows, lanes[part]] = mid + KAPPA * (value - 6.0 * mid)
            return carry

        lax.fori_loop(0, plane // 128, block, 0)

    def first(t, carry):
        one_plane(f0, t + 1, t, f1, t)
        return carry

    lax.fori_loop(0, planes + 2, first, 0)

    def second(t, carry):
        one_plane(f1, t + 1, t + 1, f0, t)
        return carry

    lax.fori_loop(0, planes, second, 0)

    def put(k, carry):
        out_ref[k] = f0[k].astype(out_ref.dtype)
        return carry

    lax.fori_loop(0, 3 * planes, put, 0)


def product_kernel(groups, rows, count, scale, order_ref, cos_ref, sin_ref, smeared_ref, *rest):
    plane = LY * LZ
    raw_refs = rest[:groups]
    out_refs = rest[groups : 2 * groups]
    sides = (rest[2 * groups : 2 * groups + 2], rest[2 * groups + 2 : 2 * groups + 4])
    total = rest[2 * groups + 4]
    chunks = smeared_ref.shape[0]
    total[...] = jnp.zeros_like(total)
    per = max(1, 256 // rows)

    def fill(k, right):
        for u in range(groups):
            raw = raw_refs[u][k]
            first = 2 * rows * u
            right[first : first + rows, :] = raw
            right[first + rows : first + 2 * rows, 0:plane] = -raw[:, plane:]
            right[first + rows : first + 2 * rows, plane:] = raw[:, :plane]

    def turn(k, left, q):
        for lane in range(0, plane, 128):
            cosine = cos_ref[k // 3, q : q + 1, lane : lane + 128]
            sine = sin_ref[k // 3, q : q + 1, lane : lane + 128]
            for row in range(0, rows, 16):
                sr = smeared_ref[k, row : row + 16, lane : lane + 128].astype(jnp.float32)
                si = smeared_ref[k, row : row + 16, plane + lane : plane + lane + 128].astype(jnp.float32)
                at = slice(q * rows + row, q * rows + row + 16)
                left[at, lane : lane + 128] = (cosine * sr + sine * si).astype(left.dtype)
                left[at, plane + lane : plane + lane + 128] = (cosine * si - sine * sr).astype(left.dtype)

    def stage(k, side, later, other):
        right, left = side
        for q0 in range(0, count, per):
            q1 = min(q0 + per, count)
            at = slice(q0 * rows, q1 * rows)
            part = lax.dot_general(
                right[...], left[at, :], (((1,), (1,)), ((), ())), preferred_element_type=jnp.float32
            )
            for q in range(q0, q1):
                turn(later, other[1], q)
            total[:, at] += part
        fill(later, other[0])

    fill(0, sides[0][0])
    for q in range(count):
        turn(0, sides[0][1], q)

    def two(h, carry):
        k = 2 * h
        stage(k, sides[0], jnp.minimum(k + 1, chunks - 1), sides[1])
        stage(k + 1, sides[1], jnp.minimum(k + 2, chunks - 1), sides[0])
        return carry

    lax.fori_loop(0, chunks // 2, two, 0)
    if chunks % 2:
        stage(chunks - 1, sides[0], chunks - 1, sides[1])
    for k in range(groups):
        first = pl.multiple_of(order_ref[k] * (2 * rows), 2 * rows)
        out_refs[k][...] = (total[pl.ds(first, 2 * rows), :] * scale).astype(out_refs[k].dtype)


def phase_tables(momenta, local_sites, total_x):
    plane = LY * LZ
    site = lax.axis_index("brick") * local_sites + lax.iota(jnp.int32, local_sites)
    site = site.reshape((local_sites // plane, 1, plane))
    fraction = (
        jnp.mod(momenta[None, :, 0:1] * (site // plane), total_x).astype(jnp.float32) / total_x
        + jnp.mod(momenta[None, :, 1:2] * (site // LZ % LY), LY).astype(jnp.float32) / LY
        + jnp.mod(momenta[None, :, 2:3] * (site % LZ), LZ).astype(jnp.float32) / LZ
    )
    angle = 2.0 * math.pi * fraction
    return jnp.cos(angle), jnp.sin(angle)


def shards_kernels(vectors, gauge_links, momenta):
    plane = LY * LZ
    rows, local_sites = vectors.shape[0], vectors.shape[3]
    planes = local_sites // plane
    bricks, vecs, subs = (lax.axis_size(a) for a in ("brick", "vec", "sub"))
    groups = vecs * subs
    count = momenta.shape[0]
    low = jnp.bfloat16
    wide = jnp.transpose(vectors.reshape((rows, 3, 2, planes, plane)), (3, 1, 0, 2, 4))
    wide = wide.reshape((planes * 3, rows, 2 * plane))
    raw = wide.astype(low)
    links = gauge_links.reshape((54, local_sites))
    fold = -(-54 // rows)

    def with_links(part, piece):
        piece = jnp.pad(piece.astype(low), ((0, fold * rows - 54), (0, 0)))
        return jnp.concatenate([part, piece.reshape((fold, rows, 2 * plane))], axis=0)

    below = from_behind(with_links(raw[-6:], links[:, -2 * plane :]), "brick", 1)
    above = from_behind(with_links(raw[:6], links[:, : 2 * plane]), "brick", -1)
    across = [raw] + [from_behind(raw, "vec", -kv) for kv in range(1, vecs)]
    cosines, sines = phase_tables(momenta, local_sites, bricks * planes)

    vmem = pl.BlockSpec(memory_space=pltpu.VMEM)
    smeared = pl.pallas_call(
        functools.partial(smear_kernel, planes, rows),
        out_shape=jax.ShapeDtypeStruct((planes * 3, rows, 2 * plane), low),
        in_specs=[vmem] * 4,
        out_specs=vmem,
        scratch_shapes=[
            pltpu.VMEM((planes + 3, fold * rows, plane), jnp.float32),
            pltpu.VMEM((planes + 2, 108, 8, plane), jnp.float32),
            pltpu.VMEM(((planes + 4) * 3, rows, 2 * plane), jnp.float32),
            pltpu.VMEM(((planes + 2) * 3, rows, 2 * plane), jnp.float32),
            pltpu.VMEM((4, 3, rows, 2 * plane), jnp.float32),
        ],
        compiler_params=pltpu.CompilerParams(vmem_limit_bytes=48 * 2**20),
        cost_estimate=pl.CostEstimate(
            flops=432 * 2 * (planes + 1) * plane * rows * 4, bytes_accessed=4 * 2**20, transcendentals=0
        ),
        name="smear",
    )(wide, below, above, links)
    *across, smeared = lax.optimization_barrier((*across, smeared))
    gathered = []
    for one in across:
        for ks in range(subs):
            gathered.append(one if ks == 0 else from_behind(one, "sub", -ks))

    me_vec, me_sub, me_brick = (lax.axis_index(a) for a in ("vec", "sub", "brick"))
    owner = (me_brick + lax.iota(jnp.int32, groups)) % groups
    order = (owner // subs - me_vec) % vecs * subs + (owner % subs - me_sub) % subs
    scale = (3.0 * bricks * local_sites) ** (-0.5)
    blocks = pl.pallas_call(
        functools.partial(product_kernel, groups, rows, count, scale),
        out_shape=[jax.ShapeDtypeStruct((2 * rows, count * rows), low)] * groups,
        in_specs=[pl.BlockSpec(memory_space=pltpu.SMEM)] + [vmem] * (3 + groups),
        out_specs=[vmem] * groups,
        scratch_shapes=[
            pltpu.VMEM((2 * rows * groups, 2 * plane), low),
            pltpu.VMEM((count * rows, 2 * plane), low),
            pltpu.VMEM((2 * rows * groups, 2 * plane), low),
            pltpu.VMEM((count * rows, 2 * plane), low),
            pltpu.VMEM((2 * rows * groups, count * rows), jnp.float32),
        ],
        compiler_params=pltpu.CompilerParams(vmem_limit_bytes=40 * 2**20),
        cost_estimate=pl.CostEstimate(
            flops=2 * 2 * rows * groups * count * rows * 6 * local_sites,
            bytes_accessed=8 * 2**20,
            transcendentals=0,
        ),
        name="product",
    )(order, cosines, sines, smeared, *gathered)

    total = None
    for k in range(groups):
        pairs = [
            (b * groups + u, u * groups + (b + k) % groups)
            for b in range(bricks)
            for u in range(groups)
        ]
        got = lax.ppermute(blocks[k], ("brick", "vec", "sub"), pairs).astype(jnp.float32)
        total = got if total is None else total + got
    return jnp.transpose(total.reshape((2, rows, count, rows)), (1, 2, 0, 3))


def choose(vectors, gauge_links, momenta):
    groups = lax.axis_size(("vec", "sub"))
    planes = vectors.shape[3] // (LY * LZ)
    if groups == lax.axis_size("brick") and planes >= 2 and vectors.shape[0] % 16 == 0:
        return shards_kernels(vectors, gauge_links, momenta)
    return shards(vectors, gauge_links, momenta)


def solution(mesh):
    in_specs = (
        P(("vec", "sub"), None, None, ("grp", "brick")),
        P(None, None, None, None, ("grp", "brick")),
        P(),
    )
    out_specs = P(("vec", "sub"), "grp", None, "brick")
    return jax.shard_map(choose, mesh=mesh, in_specs=in_specs, out_specs=out_specs, check_vma=False)
```

```python
import functools
import math

import jax
import jax.numpy as jnp
from jax import lax
from jax.experimental import pallas as pl
from jax.experimental.pallas import tpu as pltpu
from jax.sharding import PartitionSpec as P

LY = 64
LZ = 8
ITERS = 2


KAPPA = 0.125


def from_behind(array, axis, by):
    peers = lax.axis_size(axis)
    return lax.ppermute(array, axis, [(i, (i + by) % peers) for i in range(peers)])


def padded_2(array, sides, width):
    for axis, dim in sides:
        peers, length = (lax.axis_size(axis), array.shape[dim])
        up = [(i, (i + 1) % peers) for i in range(peers)]
        down = [(j, i) for i, j in up]
        last = lax.slice_in_dim(array, length - width, length, axis=dim)
        initial = lax.slice_in_dim(array, 0, width, axis=dim)
        before = lax.ppermute(last, axis, up)
        after = lax.ppermute(initial, axis, down)
        array = jnp.concatenate([before, array, after], axis=dim)
    return array


def matrix_apply(matrix, source):
    matrix_real = matrix[:, :, 0][None]
    matrix_imag = matrix[:, :, 1][None]
    source_real = source[:, None, :, 0]
    source_imag = source[:, None, :, 1]
    real_part = jnp.sum(matrix_real * source_real - matrix_imag * source_imag, axis=2)
    imag_part = jnp.sum(matrix_real * source_imag + matrix_imag * source_real, axis=2)
    return jnp.stack([real_part, imag_part], axis=2)


def adjoint(matrix):
    return jnp.stack(
        [jnp.swapaxes(matrix[:, :, 0], 0, 1), -jnp.swapaxes(matrix[:, :, 1], 0, 1)], axis=2
    )


def step_depth(values, offset):
    depth_index = lax.iota(jnp.int32, values.shape[-1]) % LZ
    if offset > 0:
        return jnp.where(
            depth_index == LZ - 1, jnp.roll(values, LZ - 1, -1), jnp.roll(values, -1, -1)
        )
    return jnp.where(depth_index == 0, jnp.roll(values, 1 - LZ, -1), jnp.roll(values, 1, -1))


def step_column(values, offset):
    plane = LY * LZ
    column_index = lax.iota(jnp.int32, values.shape[-1]) // LZ % LY
    if offset > 0:
        return jnp.where(
            column_index == LY - 1, jnp.roll(values, plane - LZ, -1), jnp.roll(values, -LZ, -1)
        )
    return jnp.where(column_index == 0, jnp.roll(values, LZ - plane, -1), jnp.roll(values, LZ, -1))


def laplace_step(center, ahead, behind, here_links, back_links):
    forward = matrix_apply(here_links[0], ahead)
    backward = matrix_apply(adjoint(back_links), behind)
    total = forward + backward
    for direction, stepper in ((1, step_column), (2, step_depth)):
        forward = matrix_apply(here_links[direction], stepper(center, 1))
        backward = matrix_apply(adjoint(stepper(here_links[direction], -1)), stepper(center, -1))
        total = total + (forward + backward)
    return center + KAPPA * (total - 6.0 * center)


def shards(vectors, gauge_links, momenta):
    plane = LY * LZ
    local_sites = vectors.shape[3]
    raw_low = vectors.astype(jnp.bfloat16)
    field = vectors
    x_links = gauge_links[0]
    rim = from_behind(x_links[..., local_sites - plane :], "brick", 1)
    back_links = jnp.concatenate([rim, x_links[..., : local_sites - plane]], axis=3)
    for step in range(ITERS):
        padded = padded_2(field, (("brick", 3),), plane)
        field = laplace_step(
            padded[..., plane : plane + local_sites],
            padded[..., 2 * plane :],
            padded[..., :local_sites],
            gauge_links,
            back_links,
        )
    smeared_low = field.astype(jnp.bfloat16)
    raw_sites, smeared_sites = (
        lax.all_to_all(raw_low, ("vec", "sub"), split_axis=3, concat_axis=0, tiled=True),
        lax.all_to_all(smeared_low, ("vec", "sub"), split_axis=3, concat_axis=0, tiled=True),
    )
    groups = lax.axis_size(("vec", "sub"))
    total_vec = raw_sites.shape[0]
    width = raw_sites.shape[3]
    total_x = lax.axis_size("brick") * (local_sites // plane)
    first_site = lax.axis_index("brick") * local_sites + lax.axis_index(("vec", "sub")) * width
    site = first_site + lax.iota(jnp.int32, width)
    layer_index = (site // plane)[None]
    column_index = (site // LZ % LY)[None]
    depth_index = (site % LZ)[None]
    fraction = (
        jnp.mod(momenta[:, 0:1] * layer_index, total_x).astype(jnp.float32) / total_x
        + jnp.mod(momenta[:, 1:2] * column_index, LY).astype(jnp.float32) / LY
        + jnp.mod(momenta[:, 2:3] * depth_index, LZ).astype(jnp.float32) / LZ
    )
    angle = 2.0 * math.pi * fraction
    cosines = jnp.cos(angle)
    sines = jnp.sin(angle)
    right = smeared_sites.reshape((total_vec, 6 * width))
    scale = (3.0 * total_x * plane) ** (-0.5)

    def one_momentum(angles):
        cosine, sine = angles
        real_part = raw_sites[:, :, 0] * cosine - raw_sites[:, :, 1] * sine
        imag_part = raw_sites[:, :, 0] * sine + raw_sites[:, :, 1] * cosine
        phased = jnp.stack([real_part, imag_part], axis=2).astype(jnp.bfloat16)
        turned = jnp.stack([-phased[:, :, 1], phased[:, :, 0]], axis=2)
        left = jnp.concatenate(
            [
                phased.reshape((lax.axis_size(("vec", "sub")) * (total_vec // groups), 6 * width)),
                turned.reshape((lax.axis_size(("vec", "sub")) * (total_vec // groups), 6 * width)),
            ],
            axis=0,
        )
        product = lax.dot_general(
            left, right, (((1,), (1,)), ((), ())), preferred_element_type=jnp.float32
        )
        return product.reshape(
            (2, lax.axis_size(("vec", "sub")) * (total_vec // groups), total_vec)
        )

    blocks = lax.map(one_momentum, (cosines, sines))
    shares = lax.psum_scatter(
        jnp.transpose(blocks, (2, 0, 1, 3)) * scale, ("vec", "sub"), scatter_dimension=0, tiled=True
    )
    return lax.psum_scatter(shares, "brick", scatter_dimension=3, tiled=True)


def smear_kernel(planes, rows, x_ref, lo_ref, hi_ref, lk_ref, out_ref, stage, table, f0, f1, moved_even, moved_odd):
    plane = LY * LZ
    f32 = jnp.float32
    blocks = rows // 8
    depth = lax.broadcasted_iota(jnp.int32, (8, 128), 1) % LZ
    link_depth = lax.broadcasted_iota(jnp.int32, (stage.shape[1], plane), 1) % LZ

    for k in range(6):
        f0[k] = lo_ref[k].astype(f32)
        f0[6 + 3 * planes + k] = hi_ref[k].astype(f32)

    def take(k, carry):
        f0[6 + k] = x_ref[k]
        return carry

    lax.fori_loop(0, 3 * planes, take, 0)
    for j in range(stage.shape[1] // rows):
        at = slice(j * rows, (j + 1) * rows)
        stage[0, at] = lo_ref[6 + j, :, 0:plane].astype(f32)
        stage[1, at] = lo_ref[6 + j, :, plane:].astype(f32)
        stage[2 + planes, at] = hi_ref[6 + j, :, 0:plane].astype(f32)
    for k in range(planes):
        stage[2 + k, 0:54] = lk_ref[:, k * plane : (k + 1) * plane]

    def spread(t, carry):
        here = stage[t + 1]
        behind_x = stage[t]
        behind_y = pltpu.roll(here, LZ, 1)
        behind_z = jnp.where(
            link_depth == 0, pltpu.roll(here, plane - (LZ - 1), 1), pltpu.roll(here, 1, 1)
        )
        for r in range(54):
            table[t, r] = jnp.broadcast_to(here[r : r + 1], (8, plane))
            back = (behind_x, behind_y, behind_z)[r // 18]
            table[t, 54 + r] = jnp.broadcast_to(back[r : r + 1], (8, plane))
        return carry

    lax.fori_loop(0, planes + 2, spread, 0)

    half_blocks = blocks // 2

    def shift(source, at, k, moved):
        rows_at = pl.ds(pl.multiple_of(k % blocks * 8, 8), 8)
        first_lane = k // blocks * plane
        lanes = pl.ds(pl.multiple_of(first_lane, plane), plane)
        for c in range(3):
            v = source[at * 3 + c, rows_at, lanes]
            moved[0, c, rows_at, lanes] = pltpu.roll(v, plane - LZ, 1)
            moved[1, c, rows_at, lanes] = pltpu.roll(v, LZ, 1)
            for part in range(plane // 128):
                w = v[:, part * 128 : part * 128 + 128]
                here = pl.ds(pl.multiple_of(first_lane + part * 128, 128), 128)
                moved[2, c, rows_at, here] = jnp.where(
                    depth == LZ - 1, pltpu.roll(w, LZ - 1, 1), pltpu.roll(w, 127, 1)
                )
                moved[3, c, rows_at, here] = jnp.where(
                    depth == 0, pltpu.roll(w, 128 - (LZ - 1), 1), pltpu.roll(w, 1, 1)
                )

    def block(source, at, links, target, to, k, moved):
        lane, first = k // half_blocks, k % half_blocks * 16
        lanes = (
            pl.ds(pl.multiple_of(lane * 128, 128), 128),
            pl.ds(pl.multiple_of(plane + lane * 128, 128), 128),
        )
        at_rows = [pl.ds(pl.multiple_of(first + 8 * b, 8), 8) for b in range(2)]
        acc = {}

        def add(b, r, part, value):
            acc[b, r, part] = value + acc[b, r, part] if (b, r, part) in acc else value

        for way in range(6):
            direction, back = way // 2, way % 2
            for c in range(3):
                fields = []
                for b in range(2):
                    if direction == 0:
                        index = (at + 1 - 2 * back) * 3 + c
                        fields.append([source[index, at_rows[b], lanes[part]] for part in range(2)])
                    else:
                        fields.append([moved[way - 2, c, at_rows[b], lanes[part]] for part in range(2)])
                for r in range(3):
                    row = direction * 18 + (54 + c * 6 + r * 2 if back else r * 6 + c * 2)
                    ur = table[links, row, :, lanes[0]]
                    ui = table[links, row + 1, :, lanes[0]]
                    for b, (sr, si) in enumerate(fields):
                        if back:
                            add(b, r, 0, ur * sr + ui * si)
                            add(b, r, 1, ur * si - ui * sr)
                        else:
                            add(b, r, 0, ur * sr - ui * si)
                            add(b, r, 1, ur * si + ui * sr)
        for (b, r, part), value in acc.items():
            mid = source[at * 3 + r, at_rows[b], lanes[part]]
            target[to * 3 + r, at_rows[b], lanes[part]] = mid + KAPPA * (value - 6.0 * mid)

    def sweep(source, offset, target, count):
        trips = 2 * blocks

        def begin(k, carry):
            shift(source, 1, k, moved_even)
            return carry

        lax.fori_loop(0, trips, begin, 0)

        def one(t, now, later):
            following = jnp.minimum(t + 1, count - 1) + 1

            def trip(k, carry):
                shift(source, following, k, later)
                block(source, t + 1, t + offset, target, t, k, now)
                return carry

            lax.fori_loop(0, trips, trip, 0)

        def two(h, carry):
            one(2 * h, moved_even, moved_odd)
            one(2 * h + 1, moved_odd, moved_even)
            return carry

        lax.fori_loop(0, count // 2, two, 0)
        if count % 2:
            one(count - 1, moved_even, moved_odd)

    sweep(f0, 0, f1, planes + 2)
    sweep(f1, 1, f0, planes)

    def put(k, carry):
        out_ref[k] = f0[k].astype(out_ref.dtype)
        return carry

    lax.fori_loop(0, 3 * planes, put, 0)


def product_kernel(groups, rows, count, scale, order_ref, cos_ref, sin_ref, smeared_ref, *rest):
    plane = LY * LZ
    raw_refs = rest[:groups]
    out_refs = rest[groups : 2 * groups]
    sides = (rest[2 * groups : 2 * groups + 2], rest[2 * groups + 2 : 2 * groups + 4])
    total = rest[2 * groups + 4]
    chunks = smeared_ref.shape[0]
    total[...] = jnp.zeros_like(total)
    per = max(1, 256 // rows)

    def fill(k, right):
        for u in range(groups):
            raw = raw_refs[u][k]
            first = 2 * rows * u
            right[first : first + rows, :] = raw
            right[first + rows : first + 2 * rows, 0:plane] = -raw[:, plane:]
            right[first + rows : first + 2 * rows, plane:] = raw[:, :plane]

    def turn(k, left, q):
        for lane in range(0, plane, 128):
            cosine = cos_ref[k // 3, q : q + 1, lane : lane + 128]
            sine = sin_ref[k // 3, q : q + 1, lane : lane + 128]
            for row in range(0, rows, 16):
                sr = smeared_ref[k, row : row + 16, lane : lane + 128].astype(jnp.float32)
                si = smeared_ref[k, row : row + 16, plane + lane : plane + lane + 128].astype(jnp.float32)
                at = slice(q * rows + row, q * rows + row + 16)
                left[at, lane : lane + 128] = (cosine * sr + sine * si).astype(left.dtype)
                left[at, plane + lane : plane + lane + 128] = (cosine * si - sine * sr).astype(left.dtype)

    def stage(k, side, later, other):
        right, left = side
        for q0 in range(0, count, per):
            q1 = min(q0 + per, count)
            at = slice(q0 * rows, q1 * rows)
            part = lax.dot_general(
                right[...], left[at, :], (((1,), (1,)), ((), ())), preferred_element_type=jnp.float32
            )
            for q in range(q0, q1):
                turn(later, other[1], q)
            total[:, at] += part
        fill(later, other[0])

    fill(0, sides[0][0])
    for q in range(count):
        turn(0, sides[0][1], q)

    def two(h, carry):
        k = 2 * h
        stage(k, sides[0], jnp.minimum(k + 1, chunks - 1), sides[1])
        stage(k + 1, sides[1], jnp.minimum(k + 2, chunks - 1), sides[0])
        return carry

    lax.fori_loop(0, chunks // 2, two, 0)
    if chunks % 2:
        stage(chunks - 1, sides[0], chunks - 1, sides[1])
    for k in range(groups):
        first = pl.multiple_of(order_ref[k] * (2 * rows), 2 * rows)
        out_refs[k][...] = (total[pl.ds(first, 2 * rows), :] * scale).astype(out_refs[k].dtype)


def phase_tables(momenta, local_sites, total_x):
    plane = LY * LZ
    site = lax.axis_index("brick") * local_sites + lax.iota(jnp.int32, local_sites)
    site = site.reshape((local_sites // plane, 1, plane))
    fraction = (
        jnp.mod(momenta[None, :, 0:1] * (site // plane), total_x).astype(jnp.float32) / total_x
        + jnp.mod(momenta[None, :, 1:2] * (site // LZ % LY), LY).astype(jnp.float32) / LY
        + jnp.mod(momenta[None, :, 2:3] * (site % LZ), LZ).astype(jnp.float32) / LZ
    )
    angle = 2.0 * math.pi * fraction
    return jnp.cos(angle), jnp.sin(angle)


def shards_kernels(vectors, gauge_links, momenta):
    plane = LY * LZ
    rows, local_sites = vectors.shape[0], vectors.shape[3]
    planes = local_sites // plane
    bricks, vecs, subs = (lax.axis_size(a) for a in ("brick", "vec", "sub"))
    groups = vecs * subs
    count = momenta.shape[0]
    low = jnp.bfloat16
    wide = jnp.transpose(vectors.reshape((rows, 3, 2, planes, plane)), (3, 1, 0, 2, 4))
    wide = wide.reshape((planes * 3, rows, 2 * plane))
    raw = wide.astype(low)
    links = gauge_links.reshape((54, local_sites))
    fold = -(-54 // rows)

    def with_links(part, piece):
        piece = jnp.pad(piece.astype(low), ((0, fold * rows - 54), (0, 0)))
        return jnp.concatenate([part, piece.reshape((fold, rows, 2 * plane))], axis=0)

    below = from_behind(with_links(raw[-6:], links[:, -2 * plane :]), "brick", 1)
    above = from_behind(with_links(raw[:6], links[:, : 2 * plane]), "brick", -1)
    across = [raw] + [from_behind(raw, "vec", -kv) for kv in range(1, vecs)]
    cosines, sines = phase_tables(momenta, local_sites, bricks * planes)

    vmem = pl.BlockSpec(memory_space=pltpu.VMEM)
    smeared = pl.pallas_call(
        functools.partial(smear_kernel, planes, rows),
        out_shape=jax.ShapeDtypeStruct((planes * 3, rows, 2 * plane), low),
        in_specs=[vmem] * 4,
        out_specs=vmem,
        scratch_shapes=[
            pltpu.VMEM((planes + 3, fold * rows, plane), jnp.float32),
            pltpu.VMEM((planes + 2, 108, 8, plane), jnp.float32),
            pltpu.VMEM(((planes + 4) * 3, rows, 2 * plane), jnp.float32),
            pltpu.VMEM(((planes + 2) * 3, rows, 2 * plane), jnp.float32),
            pltpu.VMEM((4, 3, rows, 2 * plane), jnp.float32),
            pltpu.VMEM((4, 3, rows, 2 * plane), jnp.float32),
        ],
        compiler_params=pltpu.CompilerParams(vmem_limit_bytes=48 * 2**20),
        cost_estimate=pl.CostEstimate(
            flops=432 * 2 * (planes + 1) * plane * rows * 4, bytes_accessed=4 * 2**20, transcendentals=0
        ),
        name="smear",
    )(wide, below, above, links)
    *across, smeared = lax.optimization_barrier((*across, smeared))
    gathered = []
    for one in across:
        for ks in range(subs):
            gathered.append(one if ks == 0 else from_behind(one, "sub", -ks))

    me_vec, me_sub, me_brick = (lax.axis_index(a) for a in ("vec", "sub", "brick"))
    owner = (me_brick + lax.iota(jnp.int32, groups)) % groups
    order = (owner // subs - me_vec) % vecs * subs + (owner % subs - me_sub) % subs
    scale = (3.0 * bricks * local_sites) ** (-0.5)
    blocks = pl.pallas_call(
        functools.partial(product_kernel, groups, rows, count, scale),
        out_shape=[jax.ShapeDtypeStruct((2 * rows, count * rows), low)] * groups,
        in_specs=[pl.BlockSpec(memory_space=pltpu.SMEM)] + [vmem] * (3 + groups),
        out_specs=[vmem] * groups,
        scratch_shapes=[
            pltpu.VMEM((2 * rows * groups, 2 * plane), low),
            pltpu.VMEM((count * rows, 2 * plane), low),
            pltpu.VMEM((2 * rows * groups, 2 * plane), low),
            pltpu.VMEM((count * rows, 2 * plane), low),
            pltpu.VMEM((2 * rows * groups, count * rows), jnp.float32),
        ],
        compiler_params=pltpu.CompilerParams(vmem_limit_bytes=40 * 2**20),
        cost_estimate=pl.CostEstimate(
            flops=2 * 2 * rows * groups * count * rows * 6 * local_sites,
            bytes_accessed=8 * 2**20,
            transcendentals=0,
        ),
        name="product",
    )(order, cosines, sines, smeared, *gathered)

    total = None
    for k in range(groups):
        pairs = [
            (b * groups + u, u * groups + (b + k) % groups)
            for b in range(bricks)
            for u in range(groups)
        ]
        got = lax.ppermute(blocks[k], ("brick", "vec", "sub"), pairs).astype(jnp.float32)
        total = got if total is None else total + got
    return jnp.transpose(total.reshape((2, rows, count, rows)), (1, 2, 0, 3))


def choose(vectors, gauge_links, momenta):
    groups = lax.axis_size(("vec", "sub"))
    planes = vectors.shape[3] // (LY * LZ)
    if groups == lax.axis_size("brick") and planes >= 2 and vectors.shape[0] % 16 == 0:
        return shards_kernels(vectors, gauge_links, momenta)
    return shards(vectors, gauge_links, momenta)


def solution(mesh):
    in_specs = (
        P(("vec", "sub"), None, None, ("grp", "brick")),
        P(None, None, None, None, ("grp", "brick")),
        P(),
    )
    out_specs = P(("vec", "sub"), "grp", None, "brick")
    return jax.shard_map(choose, mesh=mesh, in_specs=in_specs, out_specs=out_specs, check_vma=False)
```
